32 devices in a mesh: grp: 2 (over y), dom: 16 (over z, x, core).
Axes of the slice: x: 2, y: 2, z: 4, core: 2. Of those that a mesh axis runs over, the one named last changes fastest.
Arguments:
- user_table: float32 [32768, 256], P(('grp', 'dom')), may hold values from -96 to 96
- user_accum: float32 [32768, 256], P(('grp', 'dom')), may hold values from 0.05 to 1
- item_table: float32 [32768, 256], P(('grp', 'dom')), may hold values from -11 to 11
- item_accum: float32 [32768, 256], P(('grp', 'dom')), may hold values from 0.05 to 1
- block_pick: int32 [2, 2, 32], P(None, None, ('grp', 'dom')), may hold values from 0 to 7
- positives: int32 [2, 2, 16384], P(None, None, ('grp', 'dom')), may hold values from 0 to 255
- partners: int32 [2, 16], replicated, may hold values from 0 to 15, as said below
Outputs:
- users_out: float32 [32768, 256], P(('grp', 'dom'))
- user_accum_out: float32 [32768, 256], P(('grp', 'dom'))
- items_out: float32 [32768, 256], P(('grp', 'dom'))
- item_accum_out: float32 [32768, 256], P(('grp', 'dom'))
The draws below stay inside these ranges and needn't reach their ends.
Inputs may be any that keep to these rules, and one draw needn't show every extreme that they name: partners[b, d] equals d XOR 2**j_b for one whole number j_b of 0 to log2(16) - 1 in each bucket.
All inputs are finite; a program needn't handle non-finite values.
Results may differ from the reference program's by a relative error of at most 0.0008.
Values sent between devices are 32-bit elements; how exact they have to be, the bound alone decides.
A program may use at most 64 MiB of HBM per device.

```python
import math
import jax
import jax.numpy as jnp
from jax import lax

D = 256
BLOCK = 128
BUCKETS = 2
INNER = 2
USR_DEV = 1024
ITEM_DEV = 1024
USER_SPAN = 512
USERS = 32768
ITEMS = 32768
BATCH = 256
N_GRP = 2
N_DOM = 16
DEVICES = 32


def draw_user_table(key, part):
    sub_key = jax.random.fold_in(key, 1)
    return jnp.clip(0.5 * jax.random.normal(sub_key, (USERS, D), jnp.float32), -3.0, 3.0)


def draw_item_table(key, part):
    sub_key = jax.random.fold_in(key, 2)
    return jnp.clip(0.4 * jax.random.normal(sub_key, (ITEMS, D), jnp.float32), -2.4, 2.4)


def draw_partners(key, part):
    levels = N_DOM.bit_length() - 1
    level_pick = jax.random.randint(jax.random.fold_in(key, 3), (BUCKETS, 1), 0, levels, dtype=jnp.int32)
    masks = jnp.left_shift(jnp.ones_like(level_pick), level_pick)
    groups = jnp.arange(N_DOM, dtype=jnp.int32)[None, :]
    return jnp.bitwise_xor(groups, masks).astype(jnp.int32)


def set_ends(drawn, stream_key, least, largest):
    extent = drawn.shape
    index_at = [jax.random.randint(jax.random.fold_in(stream_key, axis), (), 0, extent[axis]) for axis in range(len(extent))]
    drawn = drawn.at[tuple(index_at)].set(least)
    longest = extent.index(max(extent))
    index_at[longest] = (index_at[longest] + 1) % extent[longest]
    return drawn.at[tuple(index_at)].set(largest)


def block_levels(stream_key, extent, cuts, least, largest):
    def one(dim, shards_of):
        heights = jax.random.uniform(jax.random.fold_in(jax.random.fold_in(stream_key, 6), dim), (shards_of,), jnp.float32, least / len(cuts), largest / len(cuts))
        return jnp.repeat(jnp.exp(heights), extent[dim] // shards_of).reshape((-1,) + (1,) * (len(extent) - dim - 1))

    level = one(*cuts[0])
    for cut in cuts[1:]:
        level = level * one(*cut)
    return level


def setup_inputs(seed: int = 0) -> dict:
    seeds = jax.random.split(jax.random.key(seed), 8)
    return {
        "user_table": draw_user_table(jax.random.fold_in(seeds[7], 71), 0),
        "user_accum": jnp.clip(jnp.exp(math.log(1.0) - 2.9957323 * jax.random.uniform(seeds[1], (USERS, D), jnp.float32) ** block_levels(seeds[1], (USERS, D), ((0, 32),), -0.2, 0.2)), 0.05, 1.0),
        "item_table": draw_item_table(jax.random.fold_in(seeds[7], 71), 0),
        "item_accum": jnp.clip(jnp.exp(math.log(1.0) - 2.9957323 * jax.random.uniform(seeds[3], (ITEMS, D), jnp.float32) ** block_levels(seeds[3], (ITEMS, D), ((0, 32),), -0.2, 0.2)), 0.05, 1.0),
        "block_pick": set_ends(jax.random.randint(seeds[4], (BUCKETS, INNER, DEVICES), 0, ITEM_DEV // BLOCK), jax.random.fold_in(seeds[4], 1), 0, (ITEM_DEV // BLOCK) - 1).astype(jnp.int32),
        "positives": set_ends(jax.random.randint(seeds[5], (BUCKETS, INNER, USER_SPAN * DEVICES), 0, BATCH), jax.random.fold_in(seeds[5], 1), 0, BATCH - 1).astype(jnp.int32),
        "partners": draw_partners(jax.random.fold_in(seeds[7], 71), 0),
    }


learn_rate = 0.3
epsilon = 1e-06

def adagrad(param, accum, grad):
    accum = accum + grad * grad
    return (param - learn_rate * grad / (jnp.sqrt(accum) + epsilon), accum)

def take_block(source, picked):
    return lax.dynamic_slice_in_dim(source, (picked * BLOCK).astype(jnp.int32), BLOCK, 0)

def put_block(source, update, picked):
    return lax.dynamic_update_slice_in_dim(source, update, (picked * BLOCK).astype(jnp.int32), 0)

def group_step(operands, sub_batch):
    users, uaccum, items, iaccum, picked, targets = operands
    user_span = USR_DEV // INNER
    first_user = sub_batch * user_span
    chosen = jax.vmap(take_block)(items, picked)
    chosen_acc = jax.vmap(take_block)(iaccum, picked)
    gathered = chosen.reshape(N_GRP * BLOCK, D)
    user_rows = users[:, first_user:first_user + user_span]
    user_acc = uaccum[:, first_user:first_user + user_span]
    scores = jnp.einsum('gud,bd->gub', user_rows, gathered, precision=lax.Precision.HIGHEST)
    softmax_rows = jax.nn.softmax(scores, axis=-1)
    onehot = (targets[:, :, None] == jnp.arange(N_GRP * BLOCK, dtype=jnp.int32)[None, None, :]).astype(jnp.float32)
    score_grad = softmax_rows - onehot
    grad_user = jnp.einsum('gub,bd->gud', score_grad, gathered, precision=lax.Precision.HIGHEST)
    grad_item = jnp.einsum('gub,gud->bd', score_grad, user_rows, precision=lax.Precision.HIGHEST).reshape(N_GRP, BLOCK, D)
    new_rows, new_acc = adagrad(user_rows, user_acc, grad_user)
    users = users.at[:, first_user:first_user + user_span].set(new_rows)
    uaccum = uaccum.at[:, first_user:first_user + user_span].set(new_acc)
    new_items, new_iacc = adagrad(chosen, chosen_acc, grad_item)
    items = jax.vmap(put_block)(items, new_items, picked)
    iaccum = jax.vmap(put_block)(iaccum, new_iacc, picked)
    return (users, uaccum, items, iaccum)

def regroup(source, per_device):
    return source.reshape(N_GRP, N_DOM, per_device, D).transpose(1, 0, 2, 3)

def restore(source):
    return source.transpose(1, 0, 2, 3).reshape(-1, D)

def reference(user_table, user_accum, item_table, item_accum, block_pick, positives, partners):
    user_span = USR_DEV // INNER
    users = regroup(user_table, USR_DEV)
    uaccum = regroup(user_accum, USR_DEV)
    items = regroup(item_table, ITEM_DEV)
    iaccum = regroup(item_accum, ITEM_DEV)
    for bucket in range(BUCKETS):
        for sub_batch in range(INNER):
            picked = block_pick[bucket, sub_batch].reshape(N_GRP, N_DOM).T
            targets = positives[bucket, sub_batch].reshape(N_GRP, N_DOM, user_span).transpose(1, 0, 2)
            users, uaccum, items, iaccum = lax.map(lambda operands: group_step(operands, sub_batch), (users, uaccum, items, iaccum, picked, targets))
        partner_row = partners[bucket].astype(jnp.int32)
        items = items[partner_row]
        iaccum = iaccum[partner_row]
    return (restore(users), restore(uaccum), restore(items), restore(iaccum))
```

```python
import jax
import jax.numpy as jnp
from jax import lax
from jax.sharding import PartitionSpec as P

BLOCK = 128
BUCKETS = 2
INNER = 2


learn_rate = 0.3
epsilon = 1e-06


def adagrad(param, accum, grad):
    accum = accum + grad * grad
    return (param - learn_rate * grad / (jnp.sqrt(accum) + epsilon), accum)


def trade(block, mask):
    if mask == 0:
        return block
    return lax.ppermute(block, "dom", [(d, d ^ mask) for d in range(lax.axis_size("dom"))])


def rotate(block, shift):
    count = lax.axis_size("grp")
    return lax.ppermute(block, "grp", [(g, (g + shift) % count) for g in range(count)])


def gather(block):
    count = lax.axis_size("grp")
    if count == 2:
        return jnp.concatenate([block, rotate(block, 1)], axis=0)
    return lax.all_gather(block, "grp", axis=0, tiled=True)


def places(targets):
    count = lax.axis_size("grp")
    if count == 2:
        return (targets - lax.axis_index("grp") * BLOCK) & (count * BLOCK - 1)
    return targets


def scatter_sum(score_grad, user_rows):
    def part(columns):
        return jnp.einsum("ub,ud->bd", columns, user_rows, precision=lax.Precision.HIGH)

    if lax.axis_size("grp") == 2:
        other = rotate(part(score_grad[:, BLOCK:]), 1)
        return part(score_grad[:, :BLOCK]) + other
    return lax.psum_scatter(part(score_grad), "grp", scatter_dimension=0, tiled=True)


def train(user_rows, user_acc, chosen, chosen_acc, targets):
    gathered = gather(chosen)
    scores = jnp.einsum("ud,bd->ub", user_rows, gathered, precision=lax.Precision.HIGHEST)
    onehot = (
        places(targets)[:, None] == jnp.arange(gathered.shape[0], dtype=jnp.int32)[None, :]
    ).astype(jnp.float32)
    score_grad = jax.nn.softmax(scores, axis=-1) - onehot
    grad_item = scatter_sum(score_grad, user_rows)
    grad_user = jnp.einsum("ub,bd->ud", score_grad, gathered, precision=lax.Precision.HIGH)
    return adagrad(user_rows, user_acc, grad_user) + adagrad(chosen, chosen_acc, grad_item)


def take(table, pick):
    return lax.dynamic_slice_in_dim(table, pick * BLOCK, BLOCK, 0)


def put(table, block, pick):
    return lax.dynamic_update_slice_in_dim(table, block, pick * BLOCK, 0)


def newest(tables, updates, pick):
    found = tuple(take(table, pick) for table in tables)
    for at, blocks in updates:
        found = tuple(jnp.where(pick == at, new, old) for new, old in zip(blocks, found))
    return found


def by_level(operands, level, masks):
    branches = [lambda *arrays, mask=mask: tuple(trade(a, mask) for a in arrays) for mask in masks]
    return lax.switch(level, branches, *operands)


def body(user_table, user_accum, item_table, item_accum, block_pick, positives, partners):
    position = lax.axis_index("dom")
    count = lax.axis_size("dom")
    levels = count.bit_length() - 1
    masks = jnp.bitwise_xor(partners[:, position], position)
    level = sum((masks >> bit & 1) * bit for bit in range(levels))
    singles = [1 << bit for bit in range(levels)]
    pairs = [(low, high) for low in range(levels) for high in range(low)]
    doubles = [0] + [1 << low | 1 << high for low, high in pairs]
    both = masks[0] ^ masks[1]
    route = sum(jnp.where(both == mask, at, 0) for at, mask in enumerate(doubles))

    picks = block_pick[:, :, 0]
    all_picks = lax.all_gather(picks, "dom", axis=0)
    wanted = all_picks[position ^ masks[0]]
    last_picks = all_picks[position ^ masks[1]]
    tables = (item_table, item_accum)
    users = list(jnp.split(user_table, INNER))
    uaccs = list(jnp.split(user_accum, INNER))

    updates = []
    for i in range(INNER):
        pick = picks[0, i]
        rows, acc = newest(tables, updates, pick)
        users[i], uaccs[i], rows, acc = train(users[i], uaccs[i], rows, acc, positives[0, i])
        updates.append((pick, (rows, acc)))
    sent = []
    for i in range(INNER):
        sent += newest(tables, updates, wanted[1, i])
    came = by_level(sent, level[0], singles)
    full = list(tables)
    for at, blocks in updates:
        full = [put(table, block, at) for table, block in zip(full, blocks)]

    updates = []
    for i in range(INNER):
        pick = picks[1, i]
        rows, acc = came[2 * i : 2 * i + 2]
        for at, blocks in updates:
            rows, acc = (jnp.where(pick == at, new, old) for new, old in zip(blocks, (rows, acc)))
        users[i], uaccs[i], rows, acc = train(users[i], uaccs[i], rows, acc, positives[1, i])
        updates.append((pick, (rows, acc)))
    late = by_level([part for _, blocks in updates for part in blocks], level[1], singles)
    bulk = by_level(full, route, doubles)
    for i in range(INNER):
        bulk = [put(t, b, last_picks[1, i]) for t, b in zip(bulk, late[2 * i : 2 * i + 2])]
    return (jnp.concatenate(users, axis=0), jnp.concatenate(uaccs, axis=0), bulk[0], bulk[1])


def solution(mesh):
    rows = P(("grp", "dom"), None)
    columns = P(None, None, ("grp", "dom"))
    return jax.shard_map(
        body,
        mesh=mesh,
        in_specs=(rows, rows, rows, rows, columns, columns, P()),
        out_specs=(rows, rows, rows, rows),
        check_vma=False,
    )
```

```python
import functools

import jax
import jax.numpy as jnp
from jax import lax
from jax.sharding import PartitionSpec as P

BLOCK = 128
BUCKETS = 2
INNER = 2


learn_rate = 0.3
epsilon = 1e-06


def adagrad(param, accum, grad):
    accum = accum + grad * grad
    return (param - learn_rate * grad / (jnp.sqrt(accum) + epsilon), accum)


def trade(block, mask):
    if mask == 0:
        return block
    return lax.ppermute(block, "dom", [(d, d ^ mask) for d in range(lax.axis_size("dom"))])


def rotate(block, shift):
    count = lax.axis_size("grp")
    return lax.ppermute(block, "grp", [(g, (g + shift) % count) for g in range(count)])


def gather(block):
    count = lax.axis_size("grp")
    if count == 2:
        return jnp.concatenate([block, rotate(block, 1)], axis=0)
    return lax.all_gather(block, "grp", axis=0, tiled=True)


def places(targets):
    count = lax.axis_size("grp")
    if count == 2:
        return (targets - lax.axis_index("grp") * BLOCK) & (count * BLOCK - 1)
    return targets


def scatter_sum(score_grad, user_rows):
    def part(columns):
        return jnp.einsum("ub,ud->bd", columns, user_rows, precision=lax.Precision.HIGH)

    if lax.axis_size("grp") == 2:
        other = rotate(part(score_grad[:, BLOCK:]), 1)
        return part(score_grad[:, :BLOCK]) + other
    return lax.psum_scatter(part(score_grad), "grp", scatter_dimension=0, tiled=True)


def train(user_rows, user_acc, chosen, chosen_acc, targets):
    gathered = gather(chosen)
    scores = jnp.einsum("ud,bd->ub", user_rows, gathered, precision=lax.Precision.HIGHEST)
    onehot = (
        places(targets)[:, None] == jnp.arange(gathered.shape[0], dtype=jnp.int32)[None, :]
    ).astype(jnp.float32)
    score_grad = jax.nn.softmax(scores, axis=-1) - onehot
    grad_item = scatter_sum(score_grad, user_rows)
    grad_user = jnp.einsum("ub,bd->ud", score_grad, gathered, precision=lax.Precision.HIGH)
    return adagrad(user_rows, user_acc, grad_user) + adagrad(chosen, chosen_acc, grad_item)


def take(table, pick):
    return lax.dynamic_slice_in_dim(table, pick * BLOCK, BLOCK, 0)


def put(table, block, pick):
    return lax.dynamic_update_slice_in_dim(table, block, pick * BLOCK, 0)


def newest(tables, updates, pick):
    found = tuple(take(table, pick) for table in tables)
    for at, blocks in updates:
        found = tuple(jnp.where(pick == at, new, old) for new, old in zip(blocks, found))
    return found


def by_level(operands, level, masks):
    branches = [lambda *arrays, mask=mask: tuple(trade(a, mask) for a in arrays) for mask in masks]
    return lax.switch(level, branches, *operands)


def body(user_table, user_accum, item_table, item_accum, block_pick, positives, partners):
    position = lax.axis_index("dom")
    count = lax.axis_size("dom")
    levels = count.bit_length() - 1
    masks = jnp.bitwise_xor(partners[:, position], position)
    level = sum((masks >> bit & 1) * bit for bit in range(levels))
    singles = [1 << bit for bit in range(levels)]
    picks = block_pick[:, :, 0]
    wanted = by_level((picks,), level[0], singles)[0]
    tables = (item_table, item_accum)
    users = list(jnp.split(user_table, INNER))
    uaccs = list(jnp.split(user_accum, INNER))

    updates = []
    for i in range(INNER):
        pick = picks[0, i]
        rows, acc = newest(tables, updates, pick)
        users[i], uaccs[i], rows, acc = train(users[i], uaccs[i], rows, acc, positives[0, i])
        updates.append((pick, (rows, acc)))
    sent = []
    for i in range(INNER):
        sent += newest(tables, updates, wanted[1, i])
    came = by_level((jnp.concatenate(sent),), level[0], singles)[0]
    came = jnp.split(came, 2 * INNER)
    full = list(tables)
    for at, blocks in updates:
        full = [put(table, block, at) for table, block in zip(full, blocks)]

    updates = []
    for i in range(INNER):
        pick = picks[1, i]
        rows, acc = came[2 * i : 2 * i + 2]
        for at, blocks in updates:
            rows, acc = (jnp.where(pick == at, new, old) for new, old in zip(blocks, (rows, acc)))
        users[i], uaccs[i], rows, acc = train(users[i], uaccs[i], rows, acc, positives[1, i])
        updates.append((pick, (rows, acc)))
    late = jnp.concatenate([part for _, blocks in updates for part in blocks])

    def leave(first, second, table, accum, late, picks):
        return (
            trade(table, first ^ second),
            trade(accum, first ^ second),
            trade(late, second),
            trade(picks, second),
        )

    *bulk, late, last_picks = lax.switch(
        level[0] * levels + level[1],
        [functools.partial(leave, first, second) for first in singles for second in singles],
        *full,
        late,
        picks,
    )
    late = jnp.split(late, 2 * INNER)
    for i in range(INNER):
        bulk = [put(t, b, last_picks[1, i]) for t, b in zip(bulk, late[2 * i : 2 * i + 2])]
    return (jnp.concatenate(users, axis=0), jnp.concatenate(uaccs, axis=0), bulk[0], bulk[1])


def solution(mesh):
    rows = P(("grp", "dom"), None)
    columns = P(None, None, ("grp", "dom"))
    return jax.shard_map(
        body,
        mesh=mesh,
        in_specs=(rows, rows, rows, rows, columns, columns, P()),
        out_specs=(rows, rows, rows, rows),
        check_vma=False,
    )
```
